16 devices in a mesh: dp: 2 (over z), wg: 8 (over y, x, core).
Axes of the slice: x: 2, y: 2, z: 2, core: 2. Of those that a mesh axis runs over, the one named last changes fastest.
Arguments:
- hidden: bfloat16 [256, 32, 4096], P(('dp', 'wg')), parts along dimension 0
- seq_lens: int32 [256], P(('dp', 'wg')), parts along dimension 0
- route_idx: int32 [8192, 2], P(('dp', 'wg')), parts along dimension 0
- g_attn_in: bfloat16 [4096], P('wg')
- w_query: bfloat16 [4096, 4096], P('wg')
- w_key: bfloat16 [4096, 1024], P('wg')
- w_value: bfloat16 [4096, 1024], P('wg')
- w_attn_out: bfloat16 [4096, 4096], P('wg')
- g_attn_out: bfloat16 [4096], P('wg')
- g_moe_in: bfloat16 [4096], P('wg')
- w_router: bfloat16 [4096, 8], P('wg')
- w_gate: bfloat16 [8, 4096, 1024], P(None, 'wg')
- w_up: bfloat16 [8, 4096, 1024], P(None, 'wg')
- w_down: bfloat16 [8, 1024, 4096], P(None, 'wg')
- g_moe_out: bfloat16 [4096], P('wg')
Outputs:
- output 1: bfloat16 [256, 32, 4096], P(('dp', 'wg')), parts along dimension 0
- output 2: bfloat16 [256, 32, 8, 128], P(('dp', 'wg')), parts along dimension 0
- output 3: bfloat16 [256, 32, 8, 128], P(('dp', 'wg')), parts along dimension 0
There are 2 independent parts. The reference program is written for one: setup_inputs(seed, part) draws one part's arguments, and reference() takes and returns one part's arrays. A program takes and returns all parts, laid end to end along the dimension named above; an argument that names none is the same for every part.
All inputs are finite; a program needn't handle non-finite values.
Results may differ from the reference program's by a relative error of at most 0.02.
Values are sent between devices in bfloat16 or wider.
A program may use at most 1 GiB of HBM per device.

```python
import jax
import jax.numpy as jnp
from jax import lax

D_MODEL = 4096
HEADS = 32
KV_HEADS = 8
HEAD_DIM = 128
EXPERTS = 8
TOP_K = 2
FF_DIM = 1024
SEQ_LEN = 32
BATCH = 128
TOKENS_DEV = 512

SOFT_CAP = 30.0
NORM_EPS = 1e-5
ROPE_BASE = 10000.0
ATTN_SCALE = HEAD_DIM ** -0.5
GROUPS = HEADS // KV_HEADS
N_ROWS = BATCH * SEQ_LEN


def normal_weight(key_w, out_shape, w_scale):
    return (jax.random.normal(key_w, out_shape, jnp.float32) * w_scale).astype(jnp.bfloat16)


def setup_inputs(seed: int = 0, part: int = 0) -> dict:
    root_key = jax.random.key(seed)
    part_key = jax.random.fold_in(jax.random.key(seed + 1), part)
    w_keys = jax.random.split(root_key, 9)
    p_keys = jax.random.split(part_key, 7)
    in_scale = D_MODEL ** -0.5
    hidden = jax.random.normal(p_keys[0], (BATCH, SEQ_LEN, D_MODEL), jnp.float32).astype(jnp.bfloat16)
    seq_lens = jax.random.randint(p_keys[1], (BATCH,), SEQ_LEN // 4, SEQ_LEN + 1)
    len_picks = jax.random.permutation(p_keys[2], BATCH)
    seq_lens = seq_lens.at[len_picks[0]].set(SEQ_LEN).at[len_picks[1]].set(SEQ_LEN // 4).astype(jnp.int32)
    draw_a = jax.random.randint(p_keys[3], (N_ROWS,), 0, EXPERTS)
    draw_b = jax.random.randint(p_keys[4], (N_ROWS,), 0, EXPERTS)
    shift_amt = jax.random.randint(p_keys[5], (), 0, EXPERTS)
    local_pos = jnp.arange(N_ROWS) % TOKENS_DEV
    first_pick = jnp.where(local_pos < EXPERTS, (local_pos + shift_amt) % EXPERTS, jnp.minimum(draw_a, draw_b))
    second_pick = (first_pick + jax.random.randint(p_keys[6], (N_ROWS,), 1, EXPERTS)) % EXPERTS
    route_idx = jnp.stack([first_pick, second_pick], axis=1).astype(jnp.int32)
    gain_rows = (1.0 + 0.3 * jax.random.normal(w_keys[7], (4, D_MODEL), jnp.float32)).astype(jnp.bfloat16)
    return {
        'hidden': hidden,
        'seq_lens': seq_lens,
        'route_idx': route_idx,
        'g_attn_in': gain_rows[0],
        'w_query': normal_weight(w_keys[0], (D_MODEL, HEADS * HEAD_DIM), 3.0 * in_scale),
        'w_key': normal_weight(w_keys[1], (D_MODEL, KV_HEADS * HEAD_DIM), 3.0 * in_scale),
        'w_value': normal_weight(w_keys[2], (D_MODEL, KV_HEADS * HEAD_DIM), in_scale),
        'w_attn_out': normal_weight(w_keys[3], (HEADS * HEAD_DIM, D_MODEL), (HEADS * HEAD_DIM) ** -0.5),
        'g_attn_out': gain_rows[1],
        'g_moe_in': gain_rows[2],
        'w_router': normal_weight(w_keys[4], (D_MODEL, EXPERTS), in_scale),
        'w_gate': normal_weight(w_keys[5], (EXPERTS, D_MODEL, FF_DIM), in_scale),
        'w_up': normal_weight(w_keys[6], (EXPERTS, D_MODEL, FF_DIM), in_scale),
        'w_down': normal_weight(w_keys[8], (EXPERTS, FF_DIM, D_MODEL), FF_DIM ** -0.5),
        'g_moe_out': gain_rows[3],
    }


def rms_norm(values, gain_vec):
    values_f32 = values.astype(jnp.float32)
    inv_rms = lax.rsqrt(jnp.mean(values_f32 * values_f32, axis=-1, keepdims=True) + NORM_EPS)
    return values_f32 * inv_rms * gain_vec.astype(jnp.float32)


def apply_rope(values, cos_t, sin_t):
    half_dim = HEAD_DIM // 2
    values_f32 = values.astype(jnp.float32)
    first_half = values_f32[..., :half_dim]
    second_half = values_f32[..., half_dim:]
    return jnp.concatenate([first_half * cos_t - second_half * sin_t, second_half * cos_t + first_half * sin_t], axis=-1).astype(jnp.bfloat16)


def reference(hidden, seq_lens, route_idx, g_attn_in, w_query, w_key, w_value, w_attn_out, g_attn_out, g_moe_in, w_router, w_gate, w_up, w_down, g_moe_out):
    half_dim = HEAD_DIM // 2
    inv_freq = ROPE_BASE ** (-jnp.arange(half_dim, dtype=jnp.float32) * (2.0 / HEAD_DIM))
    angles = jnp.arange(SEQ_LEN, dtype=jnp.float32)[:, None] * inv_freq[None, :]
    cos_t = jnp.cos(angles)[:, None, :]
    sin_t = jnp.sin(angles)[:, None, :]
    positions = jnp.arange(SEQ_LEN)
    expert_ids = jnp.arange(EXPERTS)

    def layer_prompt(operands):
        tok_rows, length, choice = operands
        h_attn = rms_norm(tok_rows, g_attn_in).astype(jnp.bfloat16)
        q_proj = jnp.dot(h_attn, w_query, preferred_element_type=jnp.float32).astype(jnp.bfloat16)
        k_proj = jnp.dot(h_attn, w_key, preferred_element_type=jnp.float32).astype(jnp.bfloat16)
        v_proj = jnp.dot(h_attn, w_value, preferred_element_type=jnp.float32).astype(jnp.bfloat16)
        q_rope = apply_rope(q_proj.reshape(SEQ_LEN, HEADS, HEAD_DIM), cos_t, sin_t).reshape(SEQ_LEN, KV_HEADS, GROUPS, HEAD_DIM)
        k_rope = apply_rope(k_proj.reshape(SEQ_LEN, KV_HEADS, HEAD_DIM), cos_t, sin_t)
        v_heads = v_proj.reshape(SEQ_LEN, KV_HEADS, HEAD_DIM)
        scores = jnp.einsum('qkgd,skd->kgqs', q_rope.astype(jnp.float32), k_rope.astype(jnp.float32)) * ATTN_SCALE
        scores = SOFT_CAP * jnp.tanh(scores / SOFT_CAP)
        allowed = (positions[None, :] <= positions[:, None]) & (positions[None, :] < length)
        scores = jnp.where(allowed, scores, -1e30)
        attn_probs = jax.nn.softmax(scores, axis=-1).astype(jnp.bfloat16)
        context = jnp.einsum('kgqs,skd->qkgd', attn_probs.astype(jnp.float32), v_heads.astype(jnp.float32)).astype(jnp.bfloat16)
        attn_out = jnp.dot(context.reshape(SEQ_LEN, HEADS * HEAD_DIM), w_attn_out, preferred_element_type=jnp.float32)
        mid_rows = (tok_rows.astype(jnp.float32) + rms_norm(attn_out, g_attn_out)).astype(jnp.bfloat16)
        h_moe = rms_norm(mid_rows, g_moe_in).astype(jnp.bfloat16)
        router_probs = jax.nn.softmax(jnp.dot(h_moe, w_router, preferred_element_type=jnp.float32), axis=-1)
        gate_probs = jnp.take_along_axis(router_probs, choice, axis=1)
        combine = jnp.sum(gate_probs[:, :, None] * (choice[:, :, None] == expert_ids).astype(jnp.float32), axis=1)

        def expert_step(moe_acc, expert_ops):
            w_gate_e, w_up_e, w_down_e, weight_col = expert_ops
            gate_act = jnp.dot(h_moe, w_gate_e, preferred_element_type=jnp.float32)
            up_act = jnp.dot(h_moe, w_up_e, preferred_element_type=jnp.float32)
            inner_act = (jax.nn.gelu(gate_act) * up_act).astype(jnp.bfloat16)
            expert_out = jnp.dot(inner_act, w_down_e, preferred_element_type=jnp.float32)
            return moe_acc + weight_col[:, None] * expert_out, None

        moe_out = lax.scan(expert_step, jnp.zeros((SEQ_LEN, D_MODEL), jnp.float32), (w_gate, w_up, w_down, combine.T))[0]
        y_rows = (mid_rows.astype(jnp.float32) + rms_norm(moe_out, g_moe_out)).astype(jnp.bfloat16)
        return y_rows, k_rope, v_heads

    y_out, k_cache, v_cache = lax.map(layer_prompt, (hidden, seq_lens, route_idx.reshape(BATCH, SEQ_LEN, TOP_K)))
    return y_out, k_cache, v_cache
```

```python
import functools
import jax
import jax.numpy as jnp
from jax import lax
from jax.sharding import PartitionSpec as P

HEAD_DIM = 128
SOFT_CAP = 30.0
NORM_EPS = 1e-5
ROPE_BASE = 10000.0
ATTN_SCALE = HEAD_DIM ** -0.5


def dot_f32(left_op, right_op):
    return jnp.dot(left_op, right_op, preferred_element_type=jnp.float32)


def rms_norm(values, gain_vec):
    values_f32 = values.astype(jnp.float32)
    inv_rms = lax.rsqrt(jnp.mean(values_f32 * values_f32, axis=-1, keepdims=True) + NORM_EPS)
    return values_f32 * inv_rms * gain_vec.astype(jnp.float32)


def rope_tables(seq_len):
    half_dim = HEAD_DIM // 2
    inv_freq = ROPE_BASE ** (-jnp.arange(half_dim, dtype=jnp.float32) * (2.0 / HEAD_DIM))
    angles = jnp.arange(seq_len, dtype=jnp.float32)[:, None] * inv_freq[None, :]
    return jnp.cos(angles)[:, None, :], jnp.sin(angles)[:, None, :]


def apply_rope(values, cos_t, sin_t):
    half_dim = HEAD_DIM // 2
    values_f32 = values.astype(jnp.float32)
    first_half = values_f32[..., :half_dim]
    second_half = values_f32[..., half_dim:]
    return jnp.concatenate([first_half * cos_t - second_half * sin_t, second_half * cos_t + first_half * sin_t], axis=-1).astype(jnp.bfloat16)


def attend(q_groups, k_rows, v_rows, lengths):
    positions = jnp.arange(q_groups.shape[1])
    scores = jnp.einsum('bqkgd,bskd->bkgqs', q_groups, k_rows, preferred_element_type=jnp.float32) * ATTN_SCALE
    scores = SOFT_CAP * jnp.tanh(scores / SOFT_CAP)
    allowed = (positions[None, :] <= positions[:, None])[None] & (positions[None, None, :] < lengths[:, None, None])
    scores = jnp.where(allowed[:, None, None], scores, -1e30)
    attn_probs = jax.nn.softmax(scores, axis=-1).astype(jnp.bfloat16)
    return jnp.einsum('bkgqs,bskd->bqkgd', attn_probs, v_rows, preferred_element_type=jnp.float32).astype(jnp.bfloat16)


def solution(mesh):
    row_spec = P(('dp', 'wg'))
    dim0_spec = P('wg', None)
    dim1_spec = P(None, 'wg', None)

    def half_gather(shard, axis):
        n = shard.shape[axis] // 2
        part = lax.dynamic_slice_in_dim(shard, lax.axis_index('dp') * n, n, axis=axis)
        return lax.all_gather(part, ('wg', 'dp'), axis=axis, tiled=True)

    def device_fn(hidden, seq_lens, route_idx, g_attn_in, w_query, w_key, w_value, w_attn_out, g_attn_out, g_moe_in, w_router, w_gate, w_up, w_down, g_moe_out):
        n_prompts, seq_len, d_model = hidden.shape
        n_exp = w_gate.shape[0]
        n_wg = lax.axis_size('wg')
        small = jnp.concatenate([g_attn_in[None], g_attn_out[None], g_moe_in[None], g_moe_out[None], w_router.T], axis=0)
        small = lax.all_gather(small, 'wg', axis=0)
        small = small.transpose(1, 0, 2).reshape(4 + n_exp, d_model)
        tok_rows = hidden.reshape(n_prompts * seq_len, d_model)
        h_attn = rms_norm(tok_rows, small[0]).astype(jnp.bfloat16)
        k_proj = dot_f32(h_attn, half_gather(w_key, 0)).astype(jnp.bfloat16)
        v_proj = dot_f32(h_attn, half_gather(w_value, 0)).astype(jnp.bfloat16)
        q_proj = dot_f32(h_attn, half_gather(w_query, 0)).astype(jnp.bfloat16)
        n_heads = q_proj.shape[1] // HEAD_DIM
        n_kv = k_proj.shape[1] // HEAD_DIM
        cos_t, sin_t = rope_tables(seq_len)
        q_rope = apply_rope(q_proj.reshape(n_prompts, seq_len, n_heads, HEAD_DIM), cos_t, sin_t)
        k_rope = apply_rope(k_proj.reshape(n_prompts, seq_len, n_kv, HEAD_DIM), cos_t, sin_t)
        v_heads = v_proj.reshape(n_prompts, seq_len, n_kv, HEAD_DIM)
        q_groups = q_rope.reshape(n_prompts, seq_len, n_kv, n_heads // n_kv, HEAD_DIM)
        context = attend(q_groups, k_rope, v_heads, seq_lens).reshape(n_prompts * seq_len, n_heads * HEAD_DIM)
        attn_out = dot_f32(context, half_gather(w_attn_out, 0))
        mid_rows = (tok_rows.astype(jnp.float32) + rms_norm(attn_out, small[1])).astype(jnp.bfloat16)
        h_moe = rms_norm(mid_rows, small[2]).astype(jnp.bfloat16)
        router_probs = jax.nn.softmax(lax.dot_general(h_moe, small[4:], (((1,), (1,)), ((), ())), preferred_element_type=jnp.float32), axis=-1)
        exp_ids = jnp.arange(n_exp)
        chosen = (route_idx[:, :, None] == exp_ids).any(axis=1)
        combine = jnp.where(chosen, router_probs, 0.0)
        moe_out = jnp.zeros((n_prompts * seq_len, d_model), jnp.float32)
        step = 2
        for e0 in range(0, n_exp, step):
            wg_ = half_gather(w_gate[e0:e0 + step], 1)
            wu_ = half_gather(w_up[e0:e0 + step], 1)
            wd_ = half_gather(w_down[e0:e0 + step], 1)
            for i in range(step):
                act = (jax.nn.gelu(dot_f32(h_moe, wg_[i])) * dot_f32(h_moe, wu_[i])).astype(jnp.bfloat16)
                moe_out = moe_out + combine[:, e0 + i][:, None] * dot_f32(act, wd_[i])
        y_rows = (mid_rows.astype(jnp.float32) + rms_norm(moe_out, small[3])).astype(jnp.bfloat16)
        return y_rows.reshape(hidden.shape), k_rope, v_heads

    return jax.shard_map(
        device_fn,
        mesh=mesh,
        in_specs=(row_spec, row_spec, row_spec, P('wg'), dim0_spec, dim0_spec, dim0_spec, dim0_spec, P('wg'), P('wg'), dim0_spec, dim1_spec, dim1_spec, dim1_spec, P('wg')),
        out_specs=(row_spec, row_spec, row_spec),
        check_vma=False,
    )
```

```python
import functools
import jax
import jax.numpy as jnp
import numpy as np
from jax import lax
from jax.experimental import pallas as pl
from jax.experimental.pallas import tpu as pltpu
from jax.sharding import PartitionSpec as P

HEAD_DIM = 128
SOFT_CAP = 30.0
NORM_EPS = 1e-5
ROPE_BASE = 10000.0
ATTN_SCALE = HEAD_DIM ** -0.5
MESH_ID = pl.DeviceIdType.MESH
F32 = jnp.float32
BF16 = jnp.bfloat16

N_ROWS = 512
D_MODEL = 4096
COLS = 1024
HALF = 512
N_EXP = 8
N_DEV = 8
FRONT = 10
DOWN = FRONT + N_EXP
UNITS = DOWN + N_EXP
COPIES = 11
SLOTS = 18
HALVES = 8
LAST = UNITS - 1
SOON = 10
LOOK = 2
LAG = 2
EARLY = FRONT + 5
THEIRS = EARLY + N_EXP
LATE = THEIRS + 3


def rope_tables(seq_len, n_rows):
    half_dim = HEAD_DIM // 2
    inv_freq = (ROPE_BASE ** (-np.arange(half_dim, dtype=np.float64) * (2.0 / HEAD_DIM))).astype(np.float32)
    angles = (np.arange(n_rows) % seq_len).astype(np.float32)[:, None] * inv_freq[None, :]
    cos_t, sin_t = np.cos(angles.astype(np.float64)), np.sin(angles.astype(np.float64))
    return (np.concatenate([cos_t, cos_t], axis=1).astype(np.float32), np.concatenate([-sin_t, sin_t], axis=1).astype(np.float32))


def steps_of(s, pairs):
    value = jnp.int32(pairs[0][1])
    for start, other in pairs[1:]:
        value = jnp.where(s >= start, other, value)
    return value


def unit_at(s):
    return s + steps_of(s, ((0, 0), (4, 6), (5, -1), (9, 2), (10, -2), (12, 0), (LAST, -1)))


def tasks_done(s):
    s = jnp.asarray(s, jnp.int32)
    return steps_of(s, tuple(enumerate((0, 0, 0, 1, 2, 3, 4, 4, 5, 6, 7, 8, 9, 10, 13, 14, 16, 19, 21, 24, 25, 26, 28, 30, 31, 32, 33, 34))))


def stage_d_done(s):
    s = jnp.asarray(s, jnp.int32)
    count = jnp.where(s > SOON, s, jnp.maximum(s - 1, 0))
    return jnp.where(s >= LAST - 1, LAST, count)


def layer_kernel(x_hbm, gains_ref, router_ref, cos_ref, sin_ref, route_ref, lens_ref, wq_ref, wk_ref, wv_ref, wo_ref, wg_ref, wu_ref, wd_ref,
                 y_ref, k_ref, v_ref, ga_ref, gb_ref,
                 h_buf, o_buf, acc, w_a, w_b, res, u_buf, q_buf, u_mine, u_theirs, x_ref, gains, router, comb, mask, route_all,
                 send_sem, recv_sem, load_sem, ssend_sem, srecv_sem, zsend_sem, zrecv_sem):
    me = lax.axis_index('wg')
    z = lax.axis_index('dp')
    core = lax.rem(me, 2)
    x = lax.rem(lax.div(me, 2), 2)
    y = lax.div(me, 4)
    x_id = me + 2 - 4 * x
    y_id = me + 4 - 8 * y
    d_id = x_id + 4 - 8 * y
    p_id = me + 1 - 2 * core
    nbr_x, nbr_y, nbr_z, nbr_p = (z, x_id), (z, y_id), (1 - z, me), (z, p_id)

    x_load = pltpu.make_async_copy(x_hbm, x_ref, load_sem.at[0])
    x_load.start()
    barrier = pltpu.get_barrier_semaphore()
    for step in range(1, N_DEV):
        pl.semaphore_signal(barrier, inc=1, device_id=(z, lax.rem(me + step, N_DEV)), device_id_type=MESH_ID)
    pl.semaphore_signal(barrier, inc=1, device_id=nbr_z, device_id_type=MESH_ID)
    pl.semaphore_wait(barrier, N_DEV)

    def rows_of(owner, first, count, quarter):
        return pl.ds(pl.multiple_of(4 * quarter * owner + first * quarter, quarter), count * quarter)

    def copy(u, k, src, dst, device):
        slot = lax.rem(u, SLOTS)
        return pltpu.make_async_remote_copy(src_ref=src, dst_ref=dst, send_sem=send_sem.at[slot, k], recv_sem=recv_sem.at[slot, k],
                                            device_id=device, device_id_type=MESH_ID)

    d_first = 2 * (1 - z)
    d_other = 2 * z
    halves = (d_first, 2, d_first, d_other, 2)
    thirds = (1 - z, 3, 3 * (1 - z), 3 * z, 1)
    whole = (0, 4)

    my_half = pl.ds(pl.multiple_of(HALF * z, HALF), HALF)
    left, right = pl.ds(0, HALF), pl.ds(HALF, HALF)

    def views(u):
        return ((u < HALVES, ga_ref.at[u], 128, halves), ((u >= HALVES) & (u < FRONT), ga_ref.at[u], 128, thirds),
                ((u >= DOWN) & (u < LAST), gb_ref.at[u - DOWN], 32, thirds))

    def flat_views(u):
        return (is_pair(u), ga_ref.at[u], 128), (u == LAST, gb_ref.at[u - DOWN], 32)

    def is_pair(u):
        return (u >= FRONT) & (u < DOWN)

    def src_views(u):
        def cols(first):
            return pl.ds(pl.multiple_of((u - first) * COLS, COLS), COLS)

        return (
            (u == 0, wk_ref.at[:, :], ga_ref.at[u], 128, halves),
            (u == 1, wv_ref.at[:, :], ga_ref.at[u], 128, halves),
            ((u >= 2) & (u < 6), wq_ref.at[:, cols(2)], ga_ref.at[u], 128, halves),
            ((u >= 6) & (u < HALVES), wo_ref.at[:, cols(6)], ga_ref.at[u], 128, halves),
            ((u >= HALVES) & (u < FRONT), wo_ref.at[:, cols(6)], ga_ref.at[u], 128, thirds),
            ((u >= DOWN) & (u < LAST), wd_ref.at[u - DOWN], gb_ref.at[u - DOWN], 32, thirds),
            (u == LAST, wd_ref.at[u - DOWN], gb_ref.at[u - DOWN], 32, whole),
        )

    def pair_copies(u):
        e = u - FRONT
        rows = rows_of(me, 0, 4, 128)
        out = []
        for src, cols, numbers in ((wg_ref, left, (0, 1, 2)), (wu_ref, right, (5, 6, 9))):
            for number, device in zip(numbers, (nbr_x, nbr_y, nbr_p)):
                out.append(copy(u, number, src.at[e, :, my_half], ga_ref.at[u, rows, cols], device))
        return out

    def own_copies(u, src, dst, quarter, share):
        first, count = share[:2]
        part = src.at[pl.ds(pl.multiple_of(first * quarter, quarter), count * quarter)]
        to = dst.at[rows_of(me, first, count, quarter)]
        return (copy(u, 0, part, to, nbr_x), copy(u, 1, part, to, nbr_y),
                copy(u, 2, src, dst.at[rows_of(me, 0, 4, quarter)], nbr_p))

    def send_own(u):
        for cond, src, dst, quarter, share in src_views(u):
            @pl.when(cond)
            def _():
                for c in own_copies(u, src, dst, quarter, share):
                    c.start()

        @pl.when(is_pair(u))
        def _():
            for c in pair_copies(u):
                c.start()

    def same(u, k, view, rows, device):
        return copy(u, k, view.at[rows], view.at[rows], device)

    def fwd_b(u, view, quarter, share):
        give, count = share[2], share[4]
        return (same(u, 3, view, rows_of(y_id, d_first, 1, quarter), nbr_x),
                same(u, 4, view, rows_of(x_id, d_first + 1, 1, quarter), nbr_y),
                same(u, 5, view, rows_of(x_id, give, count, quarter), nbr_z),
                same(u, 6, view, rows_of(y_id, give, count, quarter), nbr_z))

    def fwd_c(u, view, quarter):
        return (same(u, 9, view, rows_of(d_id, d_first, 2, quarter), nbr_z),)

    def fwd_d(u, view, quarter):
        return (same(u, 7, view, rows_of(x_id, 0, 4, quarter), nbr_p),
                same(u, 8, view, rows_of(y_id, 0, 4, quarter), nbr_p),
                same(u, 10, view, rows_of(d_id, 0, 4, quarter), nbr_p))

    def flat_fwd_b(u, view, quarter):
        return (same(u, 3, view, rows_of(y_id, 0, 2, quarter), nbr_x), same(u, 4, view, rows_of(x_id, 2, 2, quarter), nbr_y),
                same(u, 7, view, rows_of(x_id, 0, 4, quarter), nbr_p), same(u, 8, view, rows_of(y_id, 0, 4, quarter), nbr_p))

    def flat_fwd_c(u, view, quarter):
        return (same(u, 10, view, rows_of(d_id, 0, 4, quarter), nbr_p),)

    def got(u, k, view, rows):
        same(u, k, view, rows, nbr_p).wait_recv()

    def got_half(u, k, rows, cols):
        view = ga_ref.at[u, rows, cols]
        copy(u, k, view, view, nbr_p).wait_recv()

    def stage_b(u):
        for cond, view, quarter, share in views(u):
            @pl.when(cond)
            def _():
                got(u, 0, view, rows_of(x_id, share[0], share[1], quarter))
                got(u, 1, view, rows_of(y_id, share[0], share[1], quarter))
                for c in fwd_b(u, view, quarter, share):
                    c.start()

        @pl.when(is_pair(u))
        def _():
            for owner, first in ((x_id, 0), (y_id, 1)):
                got_half(u, first, rows_of(owner, 0, 4, 128), left)
                got_half(u, first + 5, rows_of(owner, 0, 4, 128), right)

        @pl.when(u == LAST)
        def _():
            got(u, 0, gb_ref.at[u - DOWN], rows_of(x_id, 0, 4, 32))
            got(u, 1, gb_ref.at[u - DOWN], rows_of(y_id, 0, 4, 32))

        for cond, view, quarter in flat_views(u):
            @pl.when(cond)
            def _():
                for c in flat_fwd_b(u, view, quarter):
                    c.start()

    def stage_c(u):
        for cond, view, quarter, share in views(u):
            @pl.when(cond)
            def _():
                got(u, 3, view, rows_of(d_id, d_first, 1, quarter))
                got(u, 4, view, rows_of(d_id, d_first + 1, 1, quarter))
                for c in fwd_c(u, view, quarter):
                    c.start()

        for cond, view, quarter in flat_views(u):
            @pl.when(cond)
            def _():
                got(u, 3, view, rows_of(d_id, 0, 2, quarter))
                got(u, 4, view, rows_of(d_id, 2, 2, quarter))
                for c in flat_fwd_c(u, view, quarter):
                    c.start()

    def stage_d(u):
        for cond, view, quarter, share in views(u):
            @pl.when(cond)
            def _():
                got(u, 5, view, rows_of(x_id, share[3], share[4], quarter))
                got(u, 6, view, rows_of(y_id, share[3], share[4], quarter))
                got(u, 9, view, rows_of(d_id, d_other, 2, quarter))
                for c in fwd_d(u, view, quarter):
                    c.start()

    px_id, py_id, pd_id = x_id + 1 - 2 * core, y_id + 1 - 2 * core, d_id + 1 - 2 * core

    def stage_e(u):
        for cond, view, quarter, share in views(u):
            @pl.when(cond)
            def _():
                got(u, 2, view, rows_of(p_id, 0, 4, quarter))
                got(u, 7, view, rows_of(px_id, 0, 4, quarter))
                got(u, 8, view, rows_of(py_id, 0, 4, quarter))
                got(u, 10, view, rows_of(pd_id, 0, 4, quarter))
                for c in fwd_b(u, view, quarter, share) + fwd_c(u, view, quarter) + fwd_d(u, view, quarter):
                    c.wait_send()
        for cond, src, dst, quarter, share in src_views(u):
            @pl.when(cond)
            def _():
                for c in own_copies(u, src, dst, quarter, share):
                    c.wait_send()

        @pl.when(is_pair(u))
        def _():
            got_half(u, 2, rows_of(p_id, 0, 4, 128), left)
            got_half(u, 9, rows_of(p_id, 0, 4, 128), right)
            for c in pair_copies(u):
                c.wait_send()

        @pl.when(u == LAST)
        def _():
            got(u, 2, gb_ref.at[u - DOWN], rows_of(p_id, 0, 4, 32))

        for cond, view, quarter in flat_views(u):
            @pl.when(cond)
            def _():
                got(u, 7, view, rows_of(px_id, 0, 4, quarter))
                got(u, 8, view, rows_of(py_id, 0, 4, quarter))
                got(u, 10, view, rows_of(pd_id, 0, 4, quarter))
                for c in flat_fwd_b(u, view, quarter) + flat_fwd_c(u, view, quarter):
                    c.wait_send()

    def load_all(copies, dst, buf, quarter):
        for i, owner in enumerate((p_id, x_id, px_id, y_id, py_id, d_id, pd_id)):
            rows = rows_of(owner, 0, 4, quarter)
            copies.append(pltpu.make_async_copy(dst.at[rows], buf.at[rows], load_sem.at[i + 2]))
        for c in copies:
            c.start()
        for c in copies:
            c.wait()

    def load(u):
        for cond, src, dst, quarter, share in src_views(u):
            buf = w_a if quarter == 128 else w_b

            @pl.when(cond)
            def _():
                load_all([pltpu.make_async_copy(src, buf.at[rows_of(me, 0, 4, quarter)], load_sem.at[0])], dst, buf, quarter)

        @pl.when(is_pair(u))
        def _():
            rows = rows_of(me, 0, 4, 128)
            load_all([pltpu.make_async_copy(wg_ref.at[u - FRONT, :, my_half], w_a.at[rows, left], load_sem.at[0]),
                      pltpu.make_async_copy(wu_ref.at[u - FRONT, :, my_half], w_a.at[rows, right], load_sem.at[1])], ga_ref.at[u], w_a, 128)

    def z_copy(src, dst, i):
        return pltpu.make_async_remote_copy(src_ref=src, dst_ref=dst, send_sem=zsend_sem.at[i], recv_sem=zrecv_sem.at[i],
                                            device_id=nbr_z, device_id_type=MESH_ID)

    route_copy = z_copy(route_ref, route_all.at[1], 0)
    rows_copy = z_copy(h_buf.at[0], h_buf.at[1], 1)
    act_copy = z_copy(u_mine.at[1], u_theirs, 2)

    send_own(jnp.int32(0))
    send_own(jnp.int32(1))
    route_copy.start()
    route_all[0] = route_ref[...]

    my_cols = pl.ds(pl.multiple_of(me * 512, 512), 512)

    def small_copies(step, cols, device):
        return [pltpu.make_async_remote_copy(src_ref=src, dst_ref=dst.at[:, cols], send_sem=ssend_sem.at[step - 1, i],
                                             recv_sem=srecv_sem.at[step - 1, i], device_id=device, device_id_type=MESH_ID)
                for i, (src, dst) in enumerate(((gains_ref, gains), (router_ref, router)))]

    for step in range(1, N_DEV):
        for c in small_copies(step, my_cols, (z, lax.rem(me + step, N_DEV))):
            c.start()
    gains[:, my_cols] = gains_ref[...]
    router[:, my_cols] = router_ref[...]
    for step in range(1, N_DEV):
        src_id = lax.rem(me + N_DEV - step, N_DEV)
        for c in small_copies(step, pl.ds(pl.multiple_of(src_id * 512, 512), 512), nbr_p):
            c.wait_recv()
    for step in range(1, N_DEV):
        for c in small_copies(step, my_cols, (z, lax.rem(me + step, N_DEV))):
            c.wait_send()
    x_load.wait()

    def gain(i):
        return gains[pl.ds(i, 1), :].astype(F32)

    def normed(values, gain_row):
        inv = lax.rsqrt(jnp.mean(values * values, axis=-1, keepdims=True) + NORM_EPS)
        return values * inv * gain_row

    CH = 16

    def norm_rows(i, _):
        rows = pl.ds(pl.multiple_of(i * CH, CH), CH)
        h_buf[0, rows, :] = normed(x_ref[rows, :].astype(F32), gain(0)).astype(BF16)
        return 0

    lax.fori_loop(0, N_ROWS // CH, norm_rows, 0)

    lane = lax.broadcasted_iota(jnp.int32, (32, 128), 1)
    pos = lax.broadcasted_iota(jnp.int32, (32, 128), 0)
    for prompt in range(N_ROWS // 32):
        key = lane - 32 * (prompt % 4)
        mask[pl.ds(32 * prompt, 32), :] = jnp.where((key >= 0) & (key <= pos) & (key < lens_ref[prompt]), 1.0, 0.0)

    def rope_rows(i, _):
        rows = pl.ds(pl.multiple_of(i * 64, 64), 64)
        cos_t, sin_t = cos_ref[...], sin_ref[...]
        for hd in range(COLS // HEAD_DIM):
            cols = pl.ds(hd * HEAD_DIM, HEAD_DIM)
            val = res[1, rows, cols].astype(BF16).astype(F32)
            q_buf[rows, cols] = (val * cos_t + pltpu.roll(val, HEAD_DIM // 2, 1) * sin_t).astype(BF16)
        return 0

    def attend(j):
        def head(hd, _):
            cols = pl.ds(pl.multiple_of(hd * HEAD_DIM, HEAD_DIM), HEAD_DIM)
            kv = pl.ds(pl.multiple_of(2 * HEAD_DIM * j + lax.div(hd, 4) * HEAD_DIM, HEAD_DIM), HEAD_DIM)
            out_cols = pl.ds(pl.multiple_of(COLS * j + hd * HEAD_DIM, HEAD_DIM), HEAD_DIM)
            for g in range(N_ROWS // 128):
                rows = pl.ds(g * 128, 128)
                s = lax.dot_general(q_buf[rows, cols], k_ref[rows, kv], (((1,), (1,)), ((), ())), preferred_element_type=F32) * ATTN_SCALE
                s = SOFT_CAP * jnp.tanh(s / SOFT_CAP)
                s = jnp.where(mask[rows, :] > 0.5, s, -1e30)
                p = jnp.exp(s - jnp.max(s, axis=-1, keepdims=True))
                p = (p / jnp.sum(p, axis=-1, keepdims=True)).astype(BF16)
                o_buf[rows, out_cols] = jnp.dot(p, v_ref[rows, kv], preferred_element_type=F32).astype(BF16)
            return 0

        lax.fori_loop(0, COLS // HEAD_DIM, head, 0)

    def mid_rows(i, _):
        rows = pl.ds(pl.multiple_of(i * CH, CH), CH)
        mid = (x_ref[rows, :].astype(F32) + normed(acc[rows, :], gain(1))).astype(BF16)
        o_buf[rows, :] = mid
        h_buf[0, rows, :] = normed(mid.astype(F32), gain(2)).astype(BF16)
        acc[rows, :] = jnp.zeros((CH, D_MODEL), F32)
        return 0

    def route():
        logits = lax.dot_general(h_buf[0], router[...], (((1,), (1,)), ((), ())), preferred_element_type=F32)
        lane = lax.broadcasted_iota(jnp.int32, logits.shape, 1)
        pr = jnp.exp(logits - jnp.max(logits, axis=-1, keepdims=True))
        pr = pr / jnp.sum(pr, axis=-1, keepdims=True)
        lane_f = lane.astype(F32)
        pick = (route_ref[:, 0:1] == lane_f) | (route_ref[:, 1:2] == lane_f)
        comb[...] = jnp.where(pick, pr, 0.0)

    def final_rows(i, _):
        rows = pl.ds(pl.multiple_of(i * CH, CH), CH)
        y_ref[rows, :] = (o_buf[rows, :].astype(F32) + normed(acc[rows, :], gain(3))).astype(BF16)
        return 0

    TILE = 256

    def tile_of(n):
        return pl.ds(pl.multiple_of(n * TILE, TILE), TILE)

    AROWS = 64

    def compute(u, side):
        @pl.when(u < FRONT)
        def _():
            def matmul(lhs):
                def tile(n, _):
                    res[1, :, tile_of(n)] = jnp.dot(lhs[...], w_a[:, tile_of(n)], preferred_element_type=F32)
                    return 0
                lax.fori_loop(0, COLS // TILE, tile, 0)

            @pl.when(u >= 6)
            def _():
                matmul(o_buf)
                acc[:, pl.ds(pl.multiple_of((u - 6) * COLS, COLS), COLS)] = res[1]

            @pl.when(u < 6)
            def _():
                matmul(h_buf.at[0])

            @pl.when((u < 6) & (u != 1))
            def _():
                lax.fori_loop(0, N_ROWS // 64, rope_rows, 0)

            @pl.when(u == 0)
            def _():
                k_ref[...] = q_buf[...]

            @pl.when(u == 1)
            def _():
                v_ref[...] = res[1].astype(BF16)

            @pl.when((u >= 2) & (u < 6))
            def _():
                attend(u - 2)

            @pl.when(u == FRONT - 1)
            def _():
                lax.fori_loop(0, N_ROWS // CH, mid_rows, 0)
                route()
                rows_copy.start()

        @pl.when(is_pair(u))
        def _():
            e_f = (u - FRONT).astype(F32)

            def tile(n, _):
                res[1, :, tile_of(n)] = jnp.dot(h_buf[side], w_a[:, tile_of(n)], preferred_element_type=F32)
                return 0
            lax.fori_loop(0, COLS // TILE, tile, 0)

            def act(n, _):
                rows = pl.ds(pl.multiple_of(n * AROWS, AROWS), AROWS)
                val = (jax.nn.gelu(res[1, rows, left]) * res[1, rows, right]).astype(BF16)
                for choice in range(2):
                    take = jnp.broadcast_to(route_all[side, rows, choice:choice + 1] == e_f, (AROWS, HALF))
                    old = u_mine[side, choice, rows, :]
                    u_mine[side, choice, rows, :] = jnp.where(take, val.astype(F32), old.astype(F32)).astype(BF16)
                return 0
            lax.fori_loop(0, N_ROWS // AROWS, act, 0)

        @pl.when(u >= DOWN)
        def _():
            e = u - DOWN
            e_f = e.astype(F32)

            other_half = pl.ds(pl.multiple_of(HALF * (1 - z), HALF), HALF)

            def spread(n, _):
                rows = pl.ds(pl.multiple_of(n * AROWS, AROWS), AROWS)
                first = jnp.broadcast_to(route_ref[rows, 0:1] == e_f, (AROWS, HALF))
                second = jnp.broadcast_to(route_ref[rows, 1:2] == e_f, (AROWS, HALF))
                for cols, picked in ((my_half, u_mine.at[0]), (other_half, u_theirs)):
                    val = jnp.where(first, picked[0, rows, :].astype(F32), jnp.where(second, picked[1, rows, :].astype(F32), 0.0))
                    u_buf[rows, cols] = val.astype(BF16)
                return 0

            lax.fori_loop(0, N_ROWS // AROWS, spread, 0)
            lane = lax.broadcasted_iota(jnp.int32, comb.shape, 1)
            weight = jnp.sum(jnp.where(lane == e, comb[...], 0.0), axis=-1, keepdims=True)

            def tile(n, _):
                out = jnp.dot(u_buf[...], w_b[:, tile_of(n)], preferred_element_type=F32)
                acc[:, tile_of(n)] += weight * out
                return 0

            lax.fori_loop(0, D_MODEL // TILE, tile, 0)

    def step(s, _):
        arrives = (s < LAST) | (s == LAST + 1)

        @pl.when(arrives)
        def _():
            stage_b(unit_at(s))

        @pl.when((s + LOOK < LAST) | (s == LAST - 1))
        def _():
            send_own(unit_at(s + LOOK))

        def work(t, _):
            u = t - steps_of(t, ((0, 0), (EARLY, 5), (THEIRS, 8)))
            side = steps_of(t, ((0, 0), (EARLY, 1), (THEIRS, 0)))

            @pl.when((t < EARLY) | ((t >= EARLY + 5) & (t < THEIRS)) | (t >= LATE))
            def _():
                stage_e(u)

            @pl.when(t == EARLY)
            def _():
                route_copy.wait_recv()
                rows_copy.wait_recv()

            load(u)

            @pl.when(t == THEIRS)
            def _():
                act_copy.start()

            @pl.when(t == LATE)
            def _():
                act_copy.wait_recv()

            compute(u, side)
            return 0

        lax.fori_loop(tasks_done(s - 1), tasks_done(s), work, 0)

        @pl.when(arrives)
        def _():
            stage_c(unit_at(s))

        def finish(place, _):
            stage_d(unit_at(place))
            return 0

        lax.fori_loop(stage_d_done(s - 1), stage_d_done(s), finish, 0)
        return 0

    lax.fori_loop(0, UNITS + LAG, step, 0)
    for c in (route_copy, rows_copy, act_copy):
        c.wait_send()
    lax.fori_loop(0, N_ROWS // CH, final_rows, 0)


def solution(mesh):
    row_spec = P(('dp', 'wg'))
    dim0_spec = P('wg', None)
    dim1_spec = P(None, 'wg', None)

    def device_fn(hidden, seq_lens, route_idx, g_attn_in, w_query, w_key, w_value, w_attn_out, g_attn_out, g_moe_in, w_router, w_gate, w_up, w_down, g_moe_out):
        n_prompts, seq_len, d_model = hidden.shape
        gains = jnp.concatenate([g_attn_in, g_attn_out, g_moe_in, g_moe_out]).reshape(4, g_attn_in.shape[0])
        rows = hidden.reshape(n_prompts * seq_len, d_model)
        cos_t, sin_t = rope_tables(seq_len, 64)
        route = jnp.pad(route_idx.astype(F32), ((0, 0), (0, 128 - route_idx.shape[1])))
        vmem = pl.BlockSpec(memory_space=pltpu.VMEM)
        hbm = pl.BlockSpec(memory_space=pl.ANY)
        y_out, k_out, v_out, _, _ = pl.pallas_call(
            layer_kernel,
            out_shape=(
                jax.ShapeDtypeStruct((N_ROWS, D_MODEL), BF16),
                jax.ShapeDtypeStruct((N_ROWS, COLS), BF16),
                jax.ShapeDtypeStruct((N_ROWS, COLS), BF16),
                jax.ShapeDtypeStruct((DOWN, D_MODEL, COLS), BF16),
                jax.ShapeDtypeStruct((N_EXP, COLS, D_MODEL), BF16),
            ),
            in_specs=[hbm] + [vmem] * 5 + [pl.BlockSpec(memory_space=pltpu.SMEM)] + [hbm] * 7,
            out_specs=(vmem, vmem, vmem, hbm, hbm),
            scratch_shapes=[
                pltpu.VMEM((2, N_ROWS, D_MODEL), BF16),
                pltpu.VMEM((N_ROWS, D_MODEL), BF16),
                pltpu.VMEM((N_ROWS, D_MODEL), F32),
                pltpu.VMEM((D_MODEL, COLS), BF16),
                pltpu.VMEM((COLS, D_MODEL), BF16),
                pltpu.VMEM((2, N_ROWS, COLS), F32),
                pltpu.VMEM((N_ROWS, COLS), BF16),
                pltpu.VMEM((N_ROWS, COLS), BF16),
                pltpu.VMEM((2, 2, N_ROWS, HALF), BF16),
                pltpu.VMEM((2, N_ROWS, HALF), BF16),
                pltpu.VMEM((N_ROWS, D_MODEL), BF16),
                pltpu.VMEM((4, D_MODEL), BF16),
                pltpu.VMEM((N_EXP, D_MODEL), BF16),
                pltpu.VMEM((N_ROWS, N_EXP), F32),
                pltpu.VMEM((N_ROWS, 128), F32),
                pltpu.VMEM((2, N_ROWS, 128), F32),
                pltpu.SemaphoreType.DMA((SLOTS, COPIES)),
                pltpu.SemaphoreType.DMA((SLOTS, COPIES)),
                pltpu.SemaphoreType.DMA((N_DEV + 1,)),
                pltpu.SemaphoreType.DMA((N_DEV - 1, 2)),
                pltpu.SemaphoreType.DMA((N_DEV - 1, 2)),
                pltpu.SemaphoreType.DMA((3,)),
                pltpu.SemaphoreType.DMA((3,)),
            ],
            compiler_params=pltpu.CompilerParams(collective_id=0, has_side_effects=True, vmem_limit_bytes=62 * 1024 * 1024),
        )(rows, gains, w_router.T, jnp.asarray(cos_t), jnp.asarray(sin_t), route, seq_lens, w_query, w_key, w_value, w_attn_out, w_gate, w_up, w_down)
        cache_shape = (n_prompts, seq_len, COLS // HEAD_DIM, HEAD_DIM)
        return y_out.reshape(hidden.shape), k_out.reshape(cache_shape), v_out.reshape(cache_shape)

    return jax.shard_map(
        device_fn,
        mesh=mesh,
        in_specs=(row_spec, row_spec, row_spec, P('wg'), dim0_spec, dim0_spec, dim0_spec, dim0_spec, P('wg'), P('wg'), dim0_spec, dim1_spec, dim1_spec, dim1_spec, P('wg')),
        out_specs=(row_spec, row_spec, row_spec),
        check_vma=False,
    )
```

```python
import functools
import jax
import jax.numpy as jnp
import numpy as np
from jax import lax
from jax.experimental import pallas as pl
from jax.experimental.pallas import tpu as pltpu
from jax.sharding import PartitionSpec as P

HEAD_DIM = 128
SOFT_CAP = 30.0
NORM_EPS = 1e-5
ROPE_BASE = 10000.0
ATTN_SCALE = HEAD_DIM ** -0.5
MESH_ID = pl.DeviceIdType.MESH
F32 = jnp.float32
BF16 = jnp.bfloat16

N_ROWS = 512
D_MODEL = 4096
COLS = 1024
HALF = 512
N_EXP = 8
N_DEV = 8
FRONT = 10
DOWN = FRONT + N_EXP
UNITS = DOWN + N_EXP
COPIES = 11
SLOTS = 18
HALVES = 6
LAST = UNITS - 1
SOON = 10
LOOK = 2
LAG = 2
EARLY = FRONT + 5
THEIRS = EARLY + N_EXP
LATE = THEIRS + 3


def rope_tables(seq_len, n_rows):
    half_dim = HEAD_DIM // 2
    inv_freq = (ROPE_BASE ** (-np.arange(half_dim, dtype=np.float64) * (2.0 / HEAD_DIM))).astype(np.float32)
    angles = (np.arange(n_rows) % seq_len).astype(np.float32)[:, None] * inv_freq[None, :]
    cos_t, sin_t = np.cos(angles.astype(np.float64)), np.sin(angles.astype(np.float64))
    return (np.concatenate([cos_t, cos_t], axis=1).astype(np.float32), np.concatenate([-sin_t, sin_t], axis=1).astype(np.float32))


def steps_of(s, pairs):
    value = jnp.int32(pairs[0][1])
    for start, other in pairs[1:]:
        value = jnp.where(s >= start, other, value)
    return value


def unit_at(s):
    return s + steps_of(s, ((0, 0), (4, 6), (5, -1), (9, 2), (10, -2), (12, 0), (LAST, -1)))


def tasks_done(s):
    s = jnp.asarray(s, jnp.int32)
    return steps_of(s, tuple(enumerate((0, 0, 0, 1, 2, 3, 4, 4, 5, 6, 7, 8, 9, 10, 13, 14, 16, 19, 21, 24, 25, 26, 28, 30, 31, 32, 33, 34))))


def stage_d_done(s):
    s = jnp.asarray(s, jnp.int32)
    count = jnp.where(s > SOON, s, jnp.maximum(s - 1, 0))
    return jnp.where(s >= LAST - 1, LAST, count)


def layer_kernel(x_hbm, gains_ref, router_ref, cos_ref, sin_ref, route_ref, lens_ref, wq_ref, wk_ref, wv_ref, wo_ref, wg_ref, wu_ref, wd_ref,
                 y_ref, k_ref, v_ref, ga_ref, gb_ref,
                 h_buf, o_buf, acc, w_a, w_b, res, u_buf, q_buf, u_mine, u_theirs, x_ref, gains, router, comb, mask, route_all,
                 send_sem, recv_sem, load_sem, ssend_sem, srecv_sem, zsend_sem, zrecv_sem):
    me = lax.axis_index('wg')
    z = lax.axis_index('dp')
    core = lax.rem(me, 2)
    x = lax.rem(lax.div(me, 2), 2)
    y = lax.div(me, 4)
    x_id = me + 2 - 4 * x
    y_id = me + 4 - 8 * y
    d_id = x_id + 4 - 8 * y
    p_id = me + 1 - 2 * core
    nbr_x, nbr_y, nbr_z, nbr_p = (z, x_id), (z, y_id), (1 - z, me), (z, p_id)

    x_load = pltpu.make_async_copy(x_hbm, x_ref, load_sem.at[0])
    x_load.start()
    barrier = pltpu.get_barrier_semaphore()
    for step in range(1, N_DEV):
        pl.semaphore_signal(barrier, inc=1, device_id=(z, lax.rem(me + step, N_DEV)), device_id_type=MESH_ID)
    pl.semaphore_signal(barrier, inc=1, device_id=nbr_z, device_id_type=MESH_ID)
    pl.semaphore_wait(barrier, N_DEV)

    def rows_of(owner, first, count, quarter):
        return pl.ds(pl.multiple_of(4 * quarter * owner + first * quarter, quarter), count * quarter)

    def copy(u, k, src, dst, device):
        slot = lax.rem(u, SLOTS)
        return pltpu.make_async_remote_copy(src_ref=src, dst_ref=dst, send_sem=send_sem.at[slot, k], recv_sem=recv_sem.at[slot, k],
                                            device_id=device, device_id_type=MESH_ID)

    d_first = 2 * (1 - z)
    d_other = 2 * z
    halves = (d_first, 2, d_first, d_other, 2)
    thirds = (1 - z, 3, 3 * (1 - z), 3 * z, 1)
    whole = (0, 4)

    my_half = pl.ds(pl.multiple_of(HALF * z, HALF), HALF)
    left, right = pl.ds(0, HALF), pl.ds(HALF, HALF)

    def views(u):
        return ((u < HALVES, ga_ref.at[u], 128, halves), ((u >= HALVES) & (u < FRONT), ga_ref.at[u], 128, thirds),
                ((u >= DOWN) & (u < LAST), gb_ref.at[u - DOWN], 32, thirds))

    def flat_views(u):
        return (is_pair(u), ga_ref.at[u], 128), (u == LAST, gb_ref.at[u - DOWN], 32)

    def is_pair(u):
        return (u >= FRONT) & (u < DOWN)

    def src_views(u):
        def cols(first):
            return pl.ds(pl.multiple_of((u - first) * COLS, COLS), COLS)

        return (
            (u == 0, wk_ref.at[:, :], ga_ref.at[u], 128, halves),
            (u == 1, wv_ref.at[:, :], ga_ref.at[u], 128, halves),
            ((u >= 2) & (u < 6), wq_ref.at[:, cols(2)], ga_ref.at[u], 128, halves),
            ((u >= 6) & (u < HALVES), wo_ref.at[:, cols(6)], ga_ref.at[u], 128, halves),
            ((u >= HALVES) & (u < FRONT), wo_ref.at[:, cols(6)], ga_ref.at[u], 128, thirds),
            ((u >= DOWN) & (u < LAST), wd_ref.at[u - DOWN], gb_ref.at[u - DOWN], 32, thirds),
            (u == LAST, wd_ref.at[u - DOWN], gb_ref.at[u - DOWN], 32, whole),
        )

    def pair_copies(u):
        e = u - FRONT
        rows = rows_of(me, 0, 4, 128)
        out = []
        for src, cols, numbers in ((wg_ref, left, (0, 1, 2)), (wu_ref, right, (5, 6, 9))):
            for number, device in zip(numbers, (nbr_x, nbr_y, nbr_p)):
                out.append(copy(u, number, src.at[e, :, my_half], ga_ref.at[u, rows, cols], device))
        return out

    def own_copies(u, src, dst, quarter, share):
        first, count = share[:2]
        part = src.at[pl.ds(pl.multiple_of(first * quarter, quarter), count * quarter)]
        to = dst.at[rows_of(me, first, count, quarter)]
        return (copy(u, 0, part, to, nbr_x), copy(u, 1, part, to, nbr_y),
                copy(u, 2, src, dst.at[rows_of(me, 0, 4, quarter)], nbr_p))

    def send_own(u):
        for cond, src, dst, quarter, share in src_views(u):
            @pl.when(cond)
            def _():
                for c in own_copies(u, src, dst, quarter, share):
                    c.start()

        @pl.when(is_pair(u))
        def _():
            for c in pair_copies(u):
                c.start()

    def same(u, k, view, rows, device):
        return copy(u, k, view.at[rows], view.at[rows], device)

    def fwd_b(u, view, quarter, share):
        give, count = share[2], share[4]
        return (same(u, 3, view, rows_of(y_id, d_first, 1, quarter), nbr_x),
                same(u, 4, view, rows_of(x_id, d_first + 1, 1, quarter), nbr_y),
                same(u, 5, view, rows_of(x_id, give, count, quarter), nbr_z),
                same(u, 6, view, rows_of(y_id, give, count, quarter), nbr_z))

    def fwd_c(u, view, quarter):
        return (same(u, 9, view, rows_of(d_id, d_first, 2, quarter), nbr_z),)

    def fwd_d(u, view, quarter):
        return (same(u, 7, view, rows_of(x_id, 0, 4, quarter), nbr_p),
                same(u, 8, view, rows_of(y_id, 0, 4, quarter), nbr_p),
                same(u, 10, view, rows_of(d_id, 0, 4, quarter), nbr_p))

    def flat_fwd_b(u, view, quarter):
        return (same(u, 3, view, rows_of(y_id, 0, 2, quarter), nbr_x), same(u, 4, view, rows_of(x_id, 2, 2, quarter), nbr_y),
                same(u, 7, view, rows_of(x_id, 0, 4, quarter), nbr_p), same(u, 8, view, rows_of(y_id, 0, 4, quarter), nbr_p))

    def flat_fwd_c(u, view, quarter):
        return (same(u, 10, view, rows_of(d_id, 0, 4, quarter), nbr_p),)

    def got(u, k, view, rows):
        same(u, k, view, rows, nbr_p).wait_recv()

    def got_half(u, k, rows, cols):
        view = ga_ref.at[u, rows, cols]
        copy(u, k, view, view, nbr_p).wait_recv()

    def stage_b(u):
        for cond, view, quarter, share in views(u):
            @pl.when(cond)
            def _():
                got(u, 0, view, rows_of(x_id, share[0], share[1], quarter))
                got(u, 1, view, rows_of(y_id, share[0], share[1], quarter))
                for c in fwd_b(u, view, quarter, share):
                    c.start()

        @pl.when(is_pair(u))
        def _():
            for owner, first in ((x_id, 0), (y_id, 1)):
                got_half(u, first, rows_of(owner, 0, 4, 128), left)
                got_half(u, first + 5, rows_of(owner, 0, 4, 128), right)

        @pl.when(u == LAST)
        def _():
            got(u, 0, gb_ref.at[u - DOWN], rows_of(x_id, 0, 4, 32))
            got(u, 1, gb_ref.at[u - DOWN], rows_of(y_id, 0, 4, 32))

        for cond, view, quarter in flat_views(u):
            @pl.when(cond)
            def _():
                for c in flat_fwd_b(u, view, quarter):
                    c.start()

    def stage_c(u):
        for cond, view, quarter, share in views(u):
            @pl.when(cond)
            def _():
                got(u, 3, view, rows_of(d_id, d_first, 1, quarter))
                got(u, 4, view, rows_of(d_id, d_first + 1, 1, quarter))
                for c in fwd_c(u, view, quarter):
                    c.start()

        for cond, view, quarter in flat_views(u):
            @pl.when(cond)
            def _():
                got(u, 3, view, rows_of(d_id, 0, 2, quarter))
                got(u, 4, view, rows_of(d_id, 2, 2, quarter))
                for c in flat_fwd_c(u, view, quarter):
                    c.start()

    def stage_d(u):
        for cond, view, quarter, share in views(u):
            @pl.when(cond)
            def _():
                got(u, 5, view, rows_of(x_id, share[3], share[4], quarter))
                got(u, 6, view, rows_of(y_id, share[3], share[4], quarter))
                got(u, 9, view, rows_of(d_id, d_other, 2, quarter))
                for c in fwd_d(u, view, quarter):
                    c.start()

    px_id, py_id, pd_id = x_id + 1 - 2 * core, y_id + 1 - 2 * core, d_id + 1 - 2 * core

    def stage_e(u):
        for cond, view, quarter, share in views(u):
            @pl.when(cond)
            def _():
                got(u, 2, view, rows_of(p_id, 0, 4, quarter))
                got(u, 7, view, rows_of(px_id, 0, 4, quarter))
                got(u, 8, view, rows_of(py_id, 0, 4, quarter))
                got(u, 10, view, rows_of(pd_id, 0, 4, quarter))
                for c in fwd_b(u, view, quarter, share) + fwd_c(u, view, quarter) + fwd_d(u, view, quarter):
                    c.wait_send()
        for cond, src, dst, quarter, share in src_views(u):
            @pl.when(cond)
            def _():
                for c in own_copies(u, src, dst, quarter, share):
                    c.wait_send()

        @pl.when(is_pair(u))
        def _():
            got_half(u, 2, rows_of(p_id, 0, 4, 128), left)
            got_half(u, 9, rows_of(p_id, 0, 4, 128), right)
            for c in pair_copies(u):
                c.wait_send()

        @pl.when(u == LAST)
        def _():
            got(u, 2, gb_ref.at[u - DOWN], rows_of(p_id, 0, 4, 32))

        for cond, view, quarter in flat_views(u):
            @pl.when(cond)
            def _():
                got(u, 7, view, rows_of(px_id, 0, 4, quarter))
                got(u, 8, view, rows_of(py_id, 0, 4, quarter))
                got(u, 10, view, rows_of(pd_id, 0, 4, quarter))
                for c in flat_fwd_b(u, view, quarter) + flat_fwd_c(u, view, quarter):
                    c.wait_send()

    def load_all(copies, dst, buf, quarter):
        for i, owner in enumerate((p_id, x_id, px_id, y_id, py_id, d_id, pd_id)):
            rows = rows_of(owner, 0, 4, quarter)
            copies.append(pltpu.make_async_copy(dst.at[rows], buf.at[rows], load_sem.at[i + 2]))
        for c in copies:
            c.start()
        for c in copies:
            c.wait()

    def load(u):
        for cond, src, dst, quarter, share in src_views(u):
            buf = w_a if quarter == 128 else w_b

            @pl.when(cond)
            def _():
                load_all([pltpu.make_async_copy(src, buf.at[rows_of(me, 0, 4, quarter)], load_sem.at[0])], dst, buf, quarter)

        @pl.when(is_pair(u))
        def _():
            rows = rows_of(me, 0, 4, 128)
            load_all([pltpu.make_async_copy(wg_ref.at[u - FRONT, :, my_half], w_a.at[rows, left], load_sem.at[0]),
                      pltpu.make_async_copy(wu_ref.at[u - FRONT, :, my_half], w_a.at[rows, right], load_sem.at[1])], ga_ref.at[u], w_a, 128)

    def z_copy(src, dst, i):
        return pltpu.make_async_remote_copy(src_ref=src, dst_ref=dst, send_sem=zsend_sem.at[i], recv_sem=zrecv_sem.at[i],
                                            device_id=nbr_z, device_id_type=MESH_ID)

    route_copy = z_copy(route_ref, route_all.at[1], 0)
    rows_copy = z_copy(h_buf.at[0], h_buf.at[1], 1)
    act_copy = z_copy(u_mine.at[1], u_theirs, 2)

    send_own(jnp.int32(0))
    send_own(jnp.int32(1))
    route_copy.start()
    route_all[0] = route_ref[...]

    my_cols = pl.ds(pl.multiple_of(me * 512, 512), 512)

    def small_copies(step, cols, device):
        return [pltpu.make_async_remote_copy(src_ref=src, dst_ref=dst.at[:, cols], send_sem=ssend_sem.at[step - 1, i],
                                             recv_sem=srecv_sem.at[step - 1, i], device_id=device, device_id_type=MESH_ID)
                for i, (src, dst) in enumerate(((gains_ref, gains), (router_ref, router)))]

    for step in range(1, N_DEV):
        for c in small_copies(step, my_cols, (z, lax.rem(me + step, N_DEV))):
            c.start()
    gains[:, my_cols] = gains_ref[...]
    router[:, my_cols] = router_ref[...]
    for step in range(1, N_DEV):
        src_id = lax.rem(me + N_DEV - step, N_DEV)
        for c in small_copies(step, pl.ds(pl.multiple_of(src_id * 512, 512), 512), nbr_p):
            c.wait_recv()
    for step in range(1, N_DEV):
        for c in small_copies(step, my_cols, (z, lax.rem(me + step, N_DEV))):
            c.wait_send()
    x_load.wait()

    def gain(i):
        return gains[pl.ds(i, 1), :].astype(F32)

    def normed(values, gain_row):
        inv = lax.rsqrt(jnp.mean(values * values, axis=-1, keepdims=True) + NORM_EPS)
        return values * inv * gain_row

    CH = 16

    def norm_rows(i, _):
        rows = pl.ds(pl.multiple_of(i * CH, CH), CH)
        h_buf[0, rows, :] = normed(x_ref[rows, :].astype(F32), gain(0)).astype(BF16)
        return 0

    lax.fori_loop(0, N_ROWS // CH, norm_rows, 0)

    lane = lax.broadcasted_iota(jnp.int32, (32, 128), 1)
    pos = lax.broadcasted_iota(jnp.int32, (32, 128), 0)
    for prompt in range(N_ROWS // 32):
        key = lane - 32 * (prompt % 4)
        mask[pl.ds(32 * prompt, 32), :] = jnp.where((key >= 0) & (key <= pos) & (key < lens_ref[prompt]), 1.0, 0.0)

    def rope_rows(i, _):
        rows = pl.ds(pl.multiple_of(i * 64, 64), 64)
        cos_t, sin_t = cos_ref[...], sin_ref[...]
        for hd in range(COLS // HEAD_DIM):
            cols = pl.ds(hd * HEAD_DIM, HEAD_DIM)
            val = res[1, rows, cols].astype(BF16).astype(F32)
            q_buf[rows, cols] = (val * cos_t + pltpu.roll(val, HEAD_DIM // 2, 1) * sin_t).astype(BF16)
        return 0

    def attend(j):
        def head(hd, _):
            cols = pl.ds(pl.multiple_of(hd * HEAD_DIM, HEAD_DIM), HEAD_DIM)
            kv = pl.ds(pl.multiple_of(2 * HEAD_DIM * j + lax.div(hd, 4) * HEAD_DIM, HEAD_DIM), HEAD_DIM)
            out_cols = pl.ds(pl.multiple_of(COLS * j + hd * HEAD_DIM, HEAD_DIM), HEAD_DIM)
            for g in range(N_ROWS // 128):
                rows = pl.ds(g * 128, 128)
                s = lax.dot_general(q_buf[rows, cols], k_ref[rows, kv], (((1,), (1,)), ((), ())), preferred_element_type=F32) * ATTN_SCALE
                s = SOFT_CAP * jnp.tanh(s / SOFT_CAP)
                s = jnp.where(mask[rows, :] > 0.5, s, -1e30)
                p = jnp.exp(s - jnp.max(s, axis=-1, keepdims=True))
                p = (p / jnp.sum(p, axis=-1, keepdims=True)).astype(BF16)
                o_buf[rows, out_cols] = jnp.dot(p, v_ref[rows, kv], preferred_element_type=F32).astype(BF16)
            return 0

        lax.fori_loop(0, COLS // HEAD_DIM, head, 0)

    def mid_rows(i, _):
        rows = pl.ds(pl.multiple_of(i * CH, CH), CH)
        mid = (x_ref[rows, :].astype(F32) + normed(acc[rows, :], gain(1))).astype(BF16)
        o_buf[rows, :] = mid
        h_buf[0, rows, :] = normed(mid.astype(F32), gain(2)).astype(BF16)
        acc[rows, :] = jnp.zeros((CH, D_MODEL), F32)
        return 0

    def route():
        logits = lax.dot_general(h_buf[0], router[...], (((1,), (1,)), ((), ())), preferred_element_type=F32)
        lane = lax.broadcasted_iota(jnp.int32, logits.shape, 1)
        pr = jnp.exp(logits - jnp.max(logits, axis=-1, keepdims=True))
        pr = pr / jnp.sum(pr, axis=-1, keepdims=True)
        lane_f = lane.astype(F32)
        pick = (route_ref[:, 0:1] == lane_f) | (route_ref[:, 1:2] == lane_f)
        comb[...] = jnp.where(pick, pr, 0.0)

    def final_rows(i, _):
        rows = pl.ds(pl.multiple_of(i * CH, CH), CH)
        y_ref[rows, :] = (o_buf[rows, :].astype(F32) + normed(acc[rows, :], gain(3))).astype(BF16)
        return 0

    TILE = 256

    def tile_of(n):
        return pl.ds(pl.multiple_of(n * TILE, TILE), TILE)

    AROWS = 64

    def compute(u, side):
        @pl.when(u < FRONT)
        def _():
            def matmul(lhs):
                def tile(n, _):
                    res[1, :, tile_of(n)] = jnp.dot(lhs[...], w_a[:, tile_of(n)], preferred_element_type=F32)
                    return 0
                lax.fori_loop(0, COLS // TILE, tile, 0)

            @pl.when(u >= 6)
            def _():
                matmul(o_buf)
                acc[:, pl.ds(pl.multiple_of((u - 6) * COLS, COLS), COLS)] = res[1]

            @pl.when(u < 6)
            def _():
                matmul(h_buf.at[0])

            @pl.when((u < 6) & (u != 1))
            def _():
                lax.fori_loop(0, N_ROWS // 64, rope_rows, 0)

            @pl.when(u == 0)
            def _():
                k_ref[...] = q_buf[...]

            @pl.when(u == 1)
            def _():
                v_ref[...] = res[1].astype(BF16)

            @pl.when((u >= 2) & (u < 6))
            def _():
                attend(u - 2)

            @pl.when(u == FRONT - 1)
            def _():
                lax.fori_loop(0, N_ROWS // CH, mid_rows, 0)
                route()
                rows_copy.start()

        @pl.when(is_pair(u))
        def _():
            e_f = (u - FRONT).astype(F32)

            def tile(n, _):
                res[1, :, tile_of(n)] = jnp.dot(h_buf[side], w_a[:, tile_of(n)], preferred_element_type=F32)
                return 0
            lax.fori_loop(0, COLS // TILE, tile, 0)

            def act(n, _):
                rows = pl.ds(pl.multiple_of(n * AROWS, AROWS), AROWS)
                val = (jax.nn.gelu(res[1, rows, left]) * res[1, rows, right]).astype(BF16)
                for choice in range(2):
                    take = jnp.broadcast_to(route_all[side, rows, choice:choice + 1] == e_f, (AROWS, HALF))
                    old = u_mine[side, choice, rows, :]
                    u_mine[side, choice, rows, :] = jnp.where(take, val.astype(F32), old.astype(F32)).astype(BF16)
                return 0
            lax.fori_loop(0, N_ROWS // AROWS, act, 0)

        @pl.when(u >= DOWN)
        def _():
            e = u - DOWN
            e_f = e.astype(F32)

            other_half = pl.ds(pl.multiple_of(HALF * (1 - z), HALF), HALF)

            def spread(n, _):
                rows = pl.ds(pl.multiple_of(n * AROWS, AROWS), AROWS)
                first = jnp.broadcast_to(route_ref[rows, 0:1] == e_f, (AROWS, HALF))
                second = jnp.broadcast_to(route_ref[rows, 1:2] == e_f, (AROWS, HALF))
                for cols, picked in ((my_half, u_mine.at[0]), (other_half, u_theirs)):
                    val = jnp.where(first, picked[0, rows, :].astype(F32), jnp.where(second, picked[1, rows, :].astype(F32), 0.0))
                    u_buf[rows, cols] = val.astype(BF16)
                return 0

            lax.fori_loop(0, N_ROWS // AROWS, spread, 0)
            lane = lax.broadcasted_iota(jnp.int32, comb.shape, 1)
            weight = jnp.sum(jnp.where(lane == e, comb[...], 0.0), axis=-1, keepdims=True)

            def tile(n, _):
                out = jnp.dot(u_buf[...], w_b[:, tile_of(n)], preferred_element_type=F32)
                acc[:, tile_of(n)] += weight * out
                return 0

            lax.fori_loop(0, D_MODEL // TILE, tile, 0)

    def step(s, _):
        arrives = (s < LAST) | (s == LAST + 1)

        @pl.when(arrives)
        def _():
            stage_b(unit_at(s))

        @pl.when((s + LOOK < LAST) | (s == LAST - 1))
        def _():
            send_own(unit_at(s + LOOK))

        def work(t, _):
            u = t - steps_of(t, ((0, 0), (EARLY, 5), (THEIRS, 8)))
            side = steps_of(t, ((0, 0), (EARLY, 1), (THEIRS, 0)))

            @pl.when((t < EARLY) | ((t >= EARLY + 5) & (t < THEIRS)) | (t >= LATE))
            def _():
                stage_e(u)

            @pl.when(t == EARLY)
            def _():
                route_copy.wait_recv()
                rows_copy.wait_recv()

            load(u)

            @pl.when(t == THEIRS)
            def _():
                act_copy.start()

            @pl.when(t == LATE)
            def _():
                act_copy.wait_recv()

            compute(u, side)
            return 0

        lax.fori_loop(tasks_done(s - 1), tasks_done(s), work, 0)

        @pl.when(arrives)
        def _():
            stage_c(unit_at(s))

        def finish(place, _):
            stage_d(unit_at(place))
            return 0

        lax.fori_loop(stage_d_done(s - 1), stage_d_done(s), finish, 0)
        return 0

    lax.fori_loop(0, UNITS + LAG, step, 0)
    for c in (route_copy, rows_copy, act_copy):
        c.wait_send()
    lax.fori_loop(0, N_ROWS // CH, final_rows, 0)


def solution(mesh):
    row_spec = P(('dp', 'wg'))
    dim0_spec = P('wg', None)
    dim1_spec = P(None, 'wg', None)

    def device_fn(hidden, seq_lens, route_idx, g_attn_in, w_query, w_key, w_value, w_attn_out, g_attn_out, g_moe_in, w_router, w_gate, w_up, w_down, g_moe_out):
        n_prompts, seq_len, d_model = hidden.shape
        gains = jnp.concatenate([g_attn_in, g_attn_out, g_moe_in, g_moe_out]).reshape(4, g_attn_in.shape[0])
        rows = hidden.reshape(n_prompts * seq_len, d_model)
        cos_t, sin_t = rope_tables(seq_len, 64)
        route = jnp.pad(route_idx.astype(F32), ((0, 0), (0, 128 - route_idx.shape[1])))
        vmem = pl.BlockSpec(memory_space=pltpu.VMEM)
        hbm = pl.BlockSpec(memory_space=pl.ANY)
        y_out, k_out, v_out, _, _ = pl.pallas_call(
            layer_kernel,
            out_shape=(
                jax.ShapeDtypeStruct((N_ROWS, D_MODEL), BF16),
                jax.ShapeDtypeStruct((N_ROWS, COLS), BF16),
                jax.ShapeDtypeStruct((N_ROWS, COLS), BF16),
                jax.ShapeDtypeStruct((DOWN, D_MODEL, COLS), BF16),
                jax.ShapeDtypeStruct((N_EXP, COLS, D_MODEL), BF16),
            ),
            in_specs=[hbm] + [vmem] * 5 + [pl.BlockSpec(memory_space=pltpu.SMEM)] + [hbm] * 7,
            out_specs=(vmem, vmem, vmem, hbm, hbm),
            scratch_shapes=[
                pltpu.VMEM((2, N_ROWS, D_MODEL), BF16),
                pltpu.VMEM((N_ROWS, D_MODEL), BF16),
                pltpu.VMEM((N_ROWS, D_MODEL), F32),
                pltpu.VMEM((D_MODEL, COLS), BF16),
                pltpu.VMEM((COLS, D_MODEL), BF16),
                pltpu.VMEM((2, N_ROWS, COLS), F32),
                pltpu.VMEM((N_ROWS, COLS), BF16),
                pltpu.VMEM((N_ROWS, COLS), BF16),
                pltpu.VMEM((2, 2, N_ROWS, HALF), BF16),
                pltpu.VMEM((2, N_ROWS, HALF), BF16),
                pltpu.VMEM((N_ROWS, D_MODEL), BF16),
                pltpu.VMEM((4, D_MODEL), BF16),
                pltpu.VMEM((N_EXP, D_MODEL), BF16),
                pltpu.VMEM((N_ROWS, N_EXP), F32),
                pltpu.VMEM((N_ROWS, 128), F32),
                pltpu.VMEM((2, N_ROWS, 128), F32),
                pltpu.SemaphoreType.DMA((SLOTS, COPIES)),
                pltpu.SemaphoreType.DMA((SLOTS, COPIES)),
                pltpu.SemaphoreType.DMA((N_DEV + 1,)),
                pltpu.SemaphoreType.DMA((N_DEV - 1, 2)),
                pltpu.SemaphoreType.DMA((N_DEV - 1, 2)),
                pltpu.SemaphoreType.DMA((3,)),
                pltpu.SemaphoreType.DMA((3,)),
            ],
            compiler_params=pltpu.CompilerParams(collective_id=0, has_side_effects=True, vmem_limit_bytes=62 * 1024 * 1024),
        )(rows, gains, w_router.T, jnp.asarray(cos_t), jnp.asarray(sin_t), route, seq_lens, w_query, w_key, w_value, w_attn_out, w_gate, w_up, w_down)
        cache_shape = (n_prompts, seq_len, COLS // HEAD_DIM, HEAD_DIM)
        return y_out.reshape(hidden.shape), k_out.reshape(cache_shape), v_out.reshape(cache_shape)

    return jax.shard_map(
        device_fn,
        mesh=mesh,
        in_specs=(row_spec, row_spec, row_spec, P('wg'), dim0_spec, dim0_spec, dim0_spec, dim0_spec, P('wg'), P('wg'), dim0_spec, dim1_spec, dim1_spec, dim1_spec, P('wg')),
        out_specs=(row_spec, row_spec, row_spec),
        check_vma=False,
    )
```
